256 devices in a mesh: replica: 16 (over z_hi, x), shard: 16 (over y, z_lo, core).
Axes of the slice: x: 4, y: 4, z: 8 (z_hi: 4, z_lo: 2; z = z_hi * 2 + z_lo), core: 2. Of those that a mesh axis runs over, the one named last changes fastest.
Arguments:
- deltas: bfloat16 [16, 8192, 8192], P('replica', 'shard')
- master: float32 [8192, 8192], P('shard', 'replica'), may hold values from -6 to 6
- momentum: float32 [8192, 8192], P('shard', 'replica'), may hold values from -6 to 6
- block_owner: int32 [32, 1], replicated, may hold values from 0 to 15; in each aligned block of 32 rows (0 to 31, 32 to 63, ...) at most 4 rows name the same one
Outputs:
- master_out: float32 [8192, 8192], P('shard', 'replica')
- momentum_out: float32 [8192, 8192], P('shard', 'replica')
- params: bfloat16 [4096, 8192], P(None, 'replica')
The draws below stay inside these ranges and needn't reach their ends.
Inputs may be any that keep to these rules, and one draw needn't show every extreme that they name: `block_owner`: every shard owns at least one block and at most 4; some shard owns exactly 4. Rows of slots that are not live hold arbitrary deltas.
All inputs are finite; a program needn't handle non-finite values.
Results may differ from the reference program's by a relative error of at most 0.01.
Values may be sent and summed in bfloat16 or wider, within the bound.
A program may use at most 128 MiB of HBM per device.

```python
import math
import jax
import jax.numpy as jnp
import numpy as np
from jax import lax

D = 8192
BLOCK_ROWS = 128
SLOTS = 4
BLOCKS = 32
N_REPLICA = 16
N_SHARD = 16


def draw_deltas(key, part):
    rows = N_SHARD * SLOTS * BLOCK_ROWS
    base = jax.random.normal(key, (N_REPLICA, rows, D), jnp.float32)
    ramp = jnp.exp(jnp.log(3.0) * jnp.arange(rows, dtype=jnp.float32) / max(rows - 1, 1))
    rising = jnp.exp(jnp.log(3.0) * jnp.arange(N_REPLICA, dtype=jnp.float32) / max(N_REPLICA - 1, 1))
    column_ramp = jnp.exp(jnp.log(3.0) * jnp.arange(D, dtype=jnp.float32) / max(D - 1, 1))
    values = base * column_ramp[None, None, :]
    return (4.0 * values * ramp[None, :, None] * rising[:, None, None]).astype(jnp.bfloat16)


def levels(key, shape, cuts, smallest, largest):
    level, own = 1.0, jax.random.fold_in(key, 6)
    for dim, blocks in cuts:
        draws = jnp.exp(jax.random.uniform(jax.random.fold_in(own, dim), (blocks,), jnp.float32, smallest / len(cuts), largest / len(cuts)))
        level = level * jnp.repeat(draws, shape[dim] // blocks).reshape([-1 if axis == dim else 1 for axis in range(len(shape))])
    return level


def shared_out(own_key, own, number, rows, count, top, reach, slope):
    sequence = jax.random.permutation(own_key, count)
    packed, usual = load_shares(count, rows * top, reach, slope, True), load_shares(count, rows * top, reach, slope, False)
    places = jnp.arange(count)

    def named(lengths, offset_by):
        used = int((lengths > 0).sum())
        fixed = max(1, used // 4)
        moved = fixed + (places - fixed + offset_by * (used - fixed)) % max(1, count - fixed)
        return jnp.zeros((count,), jnp.int32).at[sequence[jnp.where(places < fixed, places, moved)]].set(jnp.asarray(lengths, jnp.int32))

    lengths = jnp.where(number % 4 == 0, named(packed, number // 4), named(usual, number - number // 4 - 1))
    mixed = jax.random.permutation(jax.random.fold_in(own, 3), count)
    giver, sink = mixed[0:count // 2 * 2:2], mixed[1:count // 2 * 2:2]
    slack = jnp.minimum(lengths[giver] - 1, reach - lengths[sink]) // 2
    slack = jnp.where((giver == sequence[0]) | (sink == sequence[0]) | (lengths[sink] == 0), 0, jnp.maximum(slack, 0))
    moved = jax.random.randint(jax.random.fold_in(own, 4), (count // 2,), 0, 1 << 20) % (slack + 1)
    lengths = lengths.at[giver].add(-moved).at[sink].add(moved)
    items = jnp.searchsorted(jnp.cumsum(lengths), jnp.arange(rows * top), side="right").astype(jnp.int32)
    table = items.reshape(top, rows).T
    table = table[jax.random.permutation(jax.random.fold_in(own, 1), rows)]
    offset_by = jax.random.randint(jax.random.fold_in(own, 2), (rows, 1), 0, top)
    return jnp.take_along_axis(table, (jnp.arange(top)[None, :] + offset_by) % top, axis=1)


def load_shares(number_of, total, reach, skew, full):
    loads = [(1 << 20) // math.isqrt(grade ** skew) + 1 for grade in range(1, number_of + 1)]
    largest = reach if full else min(reach, max(-(-total // number_of), total * loads[0] // sum(loads)))
    least = 1 if total - largest >= number_of - 1 else 0
    given, spare = [largest] + [least] * (number_of - 1), total - largest - least * (number_of - 1)
    while spare > 0:
        candidates = [i for i in range(1, number_of) if given[i] < largest] or [i for i in range(1, number_of) if given[i] < reach]
        whole, left = sum([loads[i] for i in candidates]), spare
        for i in candidates:
            more = min(reach - given[i], max(1, left * loads[i] // whole), spare)
            given[i] = given[i] + more
            spare = spare - more
    return np.array(given)


def normal_values(key, extent, deviation, most, cuts=(), held_as=jnp.bfloat16):
    gain = levels(key, extent, cuts, -0.22, 0.18) if cuts else 1.0
    result = jax.random.normal(key, extent, jnp.float32) * deviation * gain
    return jnp.minimum(jnp.maximum(result, -most), most).astype(held_as)


def setup_inputs(seed: int = 0) -> dict:
    arg_keys = jax.random.split(jax.random.key(seed), 5)
    deltas = draw_deltas(jax.random.fold_in(arg_keys[4], 71), 0)
    master = normal_values(arg_keys[1], (N_SHARD * SLOTS * BLOCK_ROWS, D), 1.0, 6.0, ((0, 16), (1, 16)), jnp.float32)
    momentum = normal_values(arg_keys[2], (N_SHARD * SLOTS * BLOCK_ROWS, D), 1.0, 6.0, ((0, 16), (1, 16)), jnp.float32)
    block_owner_keys = jax.random.split(jax.random.fold_in(arg_keys[3], 1), BLOCKS // BLOCKS)
    block_owner_turns = jax.random.permutation(jax.random.fold_in(arg_keys[3], 3), BLOCKS // BLOCKS)
    block_owner = jax.vmap(lambda own, number: shared_out(jax.random.fold_in(arg_keys[3], 2), own, number, BLOCKS, N_SHARD, 1, SLOTS, 2))(block_owner_keys, block_owner_turns).reshape((BLOCKS, 1))
    return dict(deltas=deltas, master=master, momentum=momentum, block_owner=block_owner)


def reference(deltas, master, momentum, block_owner):
    owner = block_owner[:, 0]
    shard_ids = jnp.arange(N_SHARD, dtype=jnp.int32)
    counts = lax.optimization_barrier(jnp.sum((owner[None, :] == shard_ids[:, None]).astype(jnp.int32), axis=1))
    live = jnp.arange(SLOTS, dtype=jnp.int32)[None, :] < counts[:, None]
    live_rows = jnp.repeat(live.reshape(-1), BLOCK_ROWS)[:, None]

    def add_one(total, piece):
        return (total + piece.astype(jnp.float32), None)
    summed, _ = lax.scan(add_one, jnp.zeros(master.shape, jnp.float32), deltas)
    avg = jnp.where(live_rows, summed / N_REPLICA, jnp.float32(0.0))
    total = jnp.sum(avg * avg)
    limit = 0.5 * jnp.sqrt(jnp.float32(BLOCKS * BLOCK_ROWS * D))
    factor = jnp.minimum(jnp.float32(1.0), limit / (jnp.sqrt(total) + 1e-06))
    grad = factor * avg
    momentum_out = jnp.where(live_rows, 0.9 * momentum + grad, momentum)
    master_out = jnp.where(live_rows, master - 0.7 * (grad + 0.9 * momentum_out), master)
    index = jnp.arange(BLOCKS, dtype=jnp.int32)
    same = (owner[None, :] == owner[:, None]) & (index[None, :] < index[:, None])
    before = lax.optimization_barrier(jnp.sum(same.astype(jnp.int32), axis=1))
    flat = (owner * SLOTS + before).astype(jnp.int32)
    blocks = master_out.reshape(N_SHARD * SLOTS, BLOCK_ROWS, D)[flat]
    params = blocks.astype(jnp.bfloat16).reshape(BLOCKS * BLOCK_ROWS, D)
    return (master_out, momentum_out, params)
```

```python
import functools

import jax
import jax.numpy as jnp
from jax import lax
from jax.experimental import pallas as pl
from jax.experimental.pallas import tpu as pltpu
from jax.sharding import Mesh
from jax.sharding import PartitionSpec as P

BLOCK_ROWS = 128
SLOTS = 4
AXES = ("zh", "x", "y", "zl", "core")
MESH = pl.DeviceIdType.MESH
NC = 8
F32 = jnp.float32
BF16 = jnp.bfloat16


def comm_kernel(
    own, delta, master, momentum,
    ha, hb, mine, tot,
    d, xr, xd, xs, zr, zd, zs, ga, gb, b32, mst, mom, n1, n2,
    load_sem, mm_sem, out_sem,
    xrs, xrr, xds, xdr, xss, xsr,
    zrs, zrr, zds, zdr, zss, zsr,
    gs, gr, hs_sem, n1s, n1r, n2s, n2r,
):
    rows = d.shape[3]
    half = rows // 2
    cols = d.shape[4]
    zh, x, y = lax.axis_index("zh"), lax.axis_index("x"), lax.axis_index("y")
    zl, core = lax.axis_index("zl"), lax.axis_index("core")
    halves = (pl.ds(0, half), pl.ds(half, half))

    def ring(i):
        return lax.rem(i + 1, 4), lax.rem(i + 3, 4), lax.rem(i + 2, 4)

    xn, zn, yn = ring(x), ring(zh), ring(y)
    xp, xm, xo = xn
    zp, zm, zo = zn
    yp, ym, yo = yn
    zl2, core2 = 1 - zl, 1 - core

    barrier = pltpu.get_barrier_semaphore()
    for peer in (
        {"x": xp}, {"x": xm}, {"zh": zp}, {"zh": zm},
        {"y": yp}, {"y": ym}, {"zl": zl2}, {"core": core2},
    ):
        pl.semaphore_signal(barrier, inc=1, device_id=peer, device_id_type=MESH)

    def row_slice(c):
        return pl.ds(pl.multiple_of(c * rows, rows), rows)

    def load(c, carry):
        for i in range(4):
            for j in range(4):
                pltpu.make_async_copy(
                    delta.at[row_slice(c), pl.ds((i * 4 + j) * cols, cols)],
                    d.at[c, i, j],
                    load_sem.at[c],
                ).start()
        return carry

    def load_mm(c):
        return (
            pltpu.make_async_copy(master.at[row_slice(c)], mst.at[c], mm_sem.at[c, 0]),
            pltpu.make_async_copy(momentum.at[row_slice(c)], mom.at[c], mm_sem.at[c, 1]),
        )

    def start_mm(c, carry):
        for copy in load_mm(c):
            copy.start()
        return carry

    lax.fori_loop(0, 2, load, 0)
    lax.fori_loop(0, 2, start_mm, 0)
    lax.fori_loop(2, NC, load, 0)
    lax.fori_loop(2, NC, start_mm, 0)

    count = jnp.int32(0)
    shard = (y * 2 + zl) * 2 + core
    for b in range(own.shape[0]):
        count = count + (own[b] == shard).astype(jnp.int32)

    pl.semaphore_wait(barrier, 8)

    def send(src, dst, ss, rs, peer):
        return pltpu.make_async_remote_copy(
            src_ref=src, dst_ref=dst, send_sem=ss, recv_sem=rs, device_id=peer, device_id_type=MESH
        )

    class Phase:
        def __init__(self, axis, near, slab, recv, sems):
            self.axis, self.near, self.slab = axis, near, slab
            self.r, self.dd, self.s = recv
            self.rs, self.rr, self.ds, self.dr, self.ss, self.sr = sems

        def relay(self, c, h):
            return send(
                self.slab(c, self.near[2], h), self.r.at[c, h],
                self.rs.at[c, h], self.rr.at[c, h], {self.axis: self.near[h]},
            )

        def direct(self, c, h):
            return send(
                self.slab(c, self.near[h], 1 - h), self.dd.at[c, h],
                self.ds.at[c, h], self.dr.at[c, h], {self.axis: self.near[h]},
            )

        def summed(self, c, h):
            return send(
                self.slab(c, self.near[h], h), self.s.at[c, h],
                self.ss.at[c, h], self.sr.at[c, h], {self.axis: self.near[h]},
            )

        def all(self, c):
            return [f(c, h) for f in (self.relay, self.direct, self.summed) for h in range(2)]

    xph = Phase(
        "x", xn, lambda c, i, h: d.at[c, :, i, halves[h], :],
        (xr, xd, xs), (xrs, xrr, xds, xdr, xss, xsr),
    )
    zph = Phase(
        "zh", zn, lambda c, i, h: d.at[c, i, x, halves[h], :],
        (zr, zd, zs), (zrs, zrr, zds, zdr, zss, zsr),
    )

    def start_x(c):
        pltpu.make_async_copy(d.at[c], d.at[c], load_sem.at[c]).wait()
        for h in range(2):
            xph.relay(c, h).start()
        for h in range(2):
            xph.direct(c, h).start()

    def sum_x(c):
        for h in range(2):
            xph.relay(c, h).wait_recv()
            for k in range(4):
                to = xn[h]
                d[c, k, to, halves[h], :] = (
                    d[c, k, to, halves[h], :].astype(F32) + xr[c, h, k].astype(F32)
                ).astype(BF16)
            xph.summed(c, h).start()

    def end_x(c):
        for h in range(2):
            xph.direct(c, h).wait_recv()
        for h in range(2):
            xph.summed(c, h).wait_recv()
        for h in range(2):
            for k in range(4):
                d[c, k, x, halves[h], :] = (
                    d[c, k, x, halves[h], :].astype(F32)
                    + xs[c, h, k].astype(F32)
                    + xd[c, 1 - h, k].astype(F32)
                ).astype(BF16)
        for h in range(2):
            zph.relay(c, h).start()
        for h in range(2):
            zph.direct(c, h).start()

    def sum_z(c):
        for h in range(2):
            zph.relay(c, h).wait_recv()
            to = zn[h]
            d[c, to, x, halves[h], :] = (
                d[c, to, x, halves[h], :].astype(F32) + zr[c, h].astype(F32)
            ).astype(BF16)
            zph.summed(c, h).start()

    def g_copy(g, k, c, i):
        up, down = g.at[ym, :, c, halves[0], :], g.at[yp, :, c, halves[1], :]
        src = (
            g.at[y, zl, c], g.at[y, zl, c], g.at[y, zl, c],
            g.at[y, zl2, c], g.at[y, zl2, c], up, down, g.at[:, :, c],
        )[i]
        dst = (ha, hb)[k].at[:, :, core, row_slice(c), :] if i == 7 else src
        peer = (
            {"zl": zl2}, {"y": yp}, {"y": ym}, {"y": yp}, {"y": ym}, {"y": yp}, {"y": ym}, {"core": core2},
        )[i]
        return send(src, dst, gs.at[k, c, i], gr.at[k, c, i], peer)

    def g_local(g, k, c):
        return pltpu.make_async_copy(
            g.at[:, :, c], (ha, hb)[k].at[:, :, core, row_slice(c), :], hs_sem.at[k, c]
        )

    def g_start(g, k, c):
        for i in (0, 1, 2):
            g_copy(g, k, c, i).start()

    def g_second(g, k, c):
        g_copy(g, k, c, 0).wait_recv()
        for i in (3, 4):
            g_copy(g, k, c, i).start()

    def g_third(g, k, c):
        for i in (1, 2, 3, 4):
            g_copy(g, k, c, i).wait_recv()
        for i in (5, 6):
            g_copy(g, k, c, i).start()

    def g_last(g, k, c):
        for i in (5, 6):
            g_copy(g, k, c, i).wait_recv()
        g_copy(g, k, c, 7).start()
        g_local(g, k, c).start()

    def mine_out(c):
        return pltpu.make_async_copy(b32.at[c], mine.at[row_slice(c)], out_sem.at[c])

    n1[zh * 4 + x] = jnp.zeros((8, 128), F32)

    def end_z(c):
        for h in range(2):
            zph.direct(c, h).wait_recv()
        for h in range(2):
            zph.summed(c, h).wait_recv()
        slot = (c * rows) // BLOCK_ROWS
        for h in range(2):
            value = (
                d[c, zh, x, halves[h], :].astype(F32)
                + zs[c, h].astype(F32)
                + zd[c, 1 - h].astype(F32)
            ) * F32(0.0625)
            value = jnp.where(slot < count, value, F32(0.0))
            b32[c, halves[h], :] = value
            gb[y, zl, c, halves[h], :] = value.astype(BF16)
            square = jnp.sum((value * value).reshape(half // 8, 8, cols), axis=0)
            part = square[:, :128]
            for k in range(1, cols // 128):
                part = part + square[:, k * 128:(k + 1) * 128]
            n1[zh * 4 + x] = n1[zh * 4 + x] + part
        g_start(gb, 1, c)
        mine_out(c).start()

    def start_a(c):
        for copy in load_mm(c):
            copy.wait()
        for h in range(2):
            ga[y, zl, c, halves[h], :] = (
                mst[c, halves[h], :] - F32(0.567) * mom[c, halves[h], :]
            ).astype(BF16)
        g_start(ga, 0, c)

    def at(t, lag, f):
        @pl.when((t >= lag) & (t < NC + lag))
        def _():
            f(t - lag)

    def loop_body(t, carry):
        at(t, 0, start_x)
        at(t, 1, sum_x)
        at(t, 2, end_x)
        at(t, 3, sum_z)
        at(t, 4, end_z)
        at(t, 0, start_a)
        at(t, 1, functools.partial(g_second, ga, 0))
        at(t, 2, functools.partial(g_third, ga, 0))
        at(t, 3, functools.partial(g_last, ga, 0))
        at(t, 5, functools.partial(g_second, gb, 1))
        at(t, 6, functools.partial(g_third, gb, 1))
        at(t, 7, functools.partial(g_last, gb, 1))
        return carry

    def norm1(i):
        r = zh * 4 + x
        q = lax.rem(r + i, 16)
        return send(n1.at[r], n1.at[r], n1s.at[i], n1r.at[i], {"zh": q // 4, "x": lax.rem(q, 4)})

    def norm2(i):
        q = lax.rem(shard + i, 16)
        return send(
            n2.at[shard], n2.at[shard], n2s.at[i], n2r.at[i],
            {"y": q // 4, "zl": lax.rem(q // 2, 2), "core": lax.rem(q, 2)},
        )

    lax.fori_loop(0, NC + 4, loop_body, 0)
    for i in range(1, 16):
        norm1(i).start()
    g_second(gb, 1, NC - 1)
    g_third(gb, 1, NC - 2)
    g_last(gb, 1, NC - 3)
    g_third(gb, 1, NC - 1)
    g_last(gb, 1, NC - 2)
    for i in range(1, 16):
        norm1(i).wait_recv()
    n2[shard] = jnp.sum(n1[...], axis=0)
    for i in range(1, 16):
        norm2(i).start()
    g_last(gb, 1, NC - 1)
    for i in range(1, 16):
        norm2(i).wait_recv()
    tot[...] = jnp.sum(n2[...], axis=0)

    for i in range(1, 16):
        norm1(i).wait_send()
        norm2(i).wait_send()

    def drain(c, carry):
        for copy in xph.all(c) + zph.all(c):
            copy.wait_send()
        for k, g in ((0, ga), (1, gb)):
            for i in range(8):
                g_copy(g, k, c, i).wait_send()
            g_copy(g, k, c, 7).wait_recv()
            g_local(g, k, c).wait()
        mine_out(c).wait()
        return carry

    lax.fori_loop(0, NC, drain, 0)


def finish_kernel(
    own, tot, ha, hb, mine, master, momentum,
    master_out, momentum_out, params,
    a, b, p, g, m, v, mo, vo, counts, sem, gsem, psem, osem,
):
    blocks = own.shape[0]
    shard = (lax.axis_index("y") * 2 + lax.axis_index("zl")) * 2 + lax.axis_index("core")
    for k in range(16):
        counts[k] = 0
    for src, dst, s in ((mine, g, 0), (master, m, 1), (momentum, v, 2)):
        pltpu.make_async_copy(src, dst, gsem.at[s]).start()

    def begin(i, carry):
        k = own[i]
        j = counts[k]
        counts[k] = j + 1
        flat = k * SLOTS + j
        pltpu.make_async_copy(ha.at[flat], a.at[i], sem.at[0, i]).start()
        pltpu.make_async_copy(hb.at[flat], b.at[i], sem.at[1, i]).start()
        return carry

    lax.fori_loop(0, blocks, begin, 0)
    limit = 0.5 * jnp.sqrt(jnp.full((1, 1), blocks * BLOCK_ROWS * params.shape[1] * 16, F32))
    total = jnp.sum(jnp.sum(tot[...], axis=0, keepdims=True), axis=1, keepdims=True)
    factor = jnp.minimum(F32(1.0), limit / (jnp.sqrt(total) + F32(1e-06)))
    scale = F32(1.33) * factor

    for src, dst, s in ((mine, g, 0), (master, m, 1), (momentum, v, 2)):
        pltpu.make_async_copy(src, dst, gsem.at[s]).wait()
    count = counts[shard]

    def update(j, carry):
        r = pl.ds(pl.multiple_of(j * 32, 32), 32)
        live = j // 4 < count
        grad = factor * g[r, :]
        old = v[r, :]
        new = jnp.where(live, F32(0.9) * old + grad, old)
        w = m[r, :]
        vo[r, :] = new
        mo[r, :] = jnp.where(live, w - F32(0.7) * (grad + F32(0.9) * new), w)
        return carry

    lax.fori_loop(0, g.shape[0] // 32, update, 0)
    pltpu.make_async_copy(mo, master_out, osem.at[0]).start()
    pltpu.make_async_copy(vo, momentum_out, osem.at[1]).start()

    def out(i):
        r = pl.ds(pl.multiple_of(i * BLOCK_ROWS, BLOCK_ROWS), BLOCK_ROWS)
        return pltpu.make_async_copy(p.at[i], params.at[r], psem.at[i])

    def block(i, carry):
        pltpu.make_async_copy(ha.at[0], a.at[i], sem.at[0, i]).wait()
        pltpu.make_async_copy(hb.at[0], b.at[i], sem.at[1, i]).wait()
        for k in range(4):
            r = pl.ds(k * 32, 32)
            p[i, r, :] = (a[i, r, :].astype(F32) - scale * b[i, r, :].astype(F32)).astype(BF16)
        out(i).start()
        return carry

    lax.fori_loop(0, blocks, block, 0)
    pltpu.make_async_copy(mo, master_out, osem.at[0]).wait()
    pltpu.make_async_copy(vo, momentum_out, osem.at[1]).wait()

    def end(i, carry):
        out(i).wait()
        return carry

    lax.fori_loop(0, blocks, end, 0)


def on_device(deltas, master, momentum, block_owner):
    rows, cols = master.shape
    part = rows // NC
    half = part // 2
    own = block_owner.reshape(-1)
    blocks = own.shape[0]
    any_spec = pl.BlockSpec(memory_space=pl.ANY)
    vmem = pl.BlockSpec(memory_space=pltpu.VMEM)
    smem = pl.BlockSpec(memory_space=pltpu.SMEM)
    sem = pltpu.SemaphoreType.DMA
    gathered = jax.ShapeDtypeStruct((4, 2, 2, rows, cols), BF16)
    ha, hb, mine, tot = pl.pallas_call(
        comm_kernel,
        name="reduce_gather",
        out_shape=(
            gathered, gathered,
            jax.ShapeDtypeStruct((rows, cols), F32),
            jax.ShapeDtypeStruct((8, 128), F32),
        ),
        in_specs=[smem, any_spec, any_spec, any_spec],
        out_specs=(any_spec, any_spec, any_spec, vmem),
        scratch_shapes=(
            [pltpu.VMEM((NC, 4, 4, part, cols), BF16)]
            + [pltpu.VMEM((NC, 2, 4, half, cols), BF16)] * 3
            + [pltpu.VMEM((NC, 2, half, cols), BF16)] * 3
            + [pltpu.VMEM((4, 2, NC, part, cols), BF16)] * 2
            + [pltpu.VMEM((NC, part, cols), F32)] * 3
            + [pltpu.VMEM((16, 8, 128), F32)] * 2
            + [sem((NC,)), sem((NC, 2)), sem((NC,))]
            + [sem((NC, 2))] * 12
            + [sem((2, NC, 8))] * 2
            + [sem((2, NC))]
            + [sem((16,))] * 4
        ),
        compiler_params=pltpu.CompilerParams(
            collective_id=0, has_side_effects=True, vmem_limit_bytes=60 * 1024 * 1024
        ),
    )(own, deltas.reshape(rows, -1), master, momentum)
    slots = 16 * SLOTS
    ha = ha.reshape(slots, BLOCK_ROWS, cols)
    hb = hb.reshape(slots, BLOCK_ROWS, cols)
    return pl.pallas_call(
        finish_kernel,
        name="finish",
        out_shape=(
            jax.ShapeDtypeStruct((rows, cols), F32),
            jax.ShapeDtypeStruct((rows, cols), F32),
            jax.ShapeDtypeStruct((blocks * BLOCK_ROWS, cols), BF16),
        ),
        in_specs=[smem, vmem] + [any_spec] * 5,
        out_specs=(any_spec, any_spec, any_spec),
        scratch_shapes=(
            [pltpu.VMEM((blocks, BLOCK_ROWS, cols), BF16)] * 3
            + [pltpu.VMEM((rows, cols), F32)] * 5
            + [pltpu.SMEM((16,), jnp.int32)]
            + [sem((2, blocks)), sem((3,)), sem((blocks,)), sem((2,))]
        ),
        compiler_params=pltpu.CompilerParams(vmem_limit_bytes=60 * 1024 * 1024),
    )(own, tot, ha, hb, mine, master, momentum)


def solution(mesh):
    finer = Mesh(mesh.devices.reshape(4, 4, 4, 2, 2), AXES)
    replica, shard = AXES[:2], AXES[2:]
    in_specs = (P(replica, shard, None), P(shard, replica), P(shard, replica), P())
    out_specs = (P(shard, replica), P(shard, replica), P(None, replica))
    return jax.shard_map(
        on_device, mesh=finer, in_specs=in_specs, out_specs=out_specs, check_vma=False
    )
```

```python
import functools

import jax
import jax.numpy as jnp
from jax import lax
from jax.experimental import pallas as pl
from jax.experimental.pallas import tpu as pltpu
from jax.sharding import Mesh
from jax.sharding import PartitionSpec as P

BLOCK_ROWS = 128
SLOTS = 4
HALF_BLOCK = 64
AXES = ("zh", "x", "y", "zl", "core")
MESH = pl.DeviceIdType.MESH
R = 32
LA = 1
F32 = jnp.float32
BF16 = jnp.bfloat16


def comm_kernel(
    nc,
    own, delta, master, momentum,
    ha, hb, tot,
    d, xt, xr, xd, xs, zr, zd, zs, ga, gb, mst, mom, axs, axr, acc, n1, n2,
    load_sem, ex_sem, mm_sem, xt_sem, ax_sem,
    xrs, xrr, xds, xdr, xss, xsr,
    zrs, zrr, zds, zdr, zss, zsr,
    gs, gr, hs_sem, n1s, n1r, n2s, n2r,
):
    chunks = d.shape[0]
    extra = chunks - nc
    per_block = BLOCK_ROWS // R
    half = R // 2
    cols = master.shape[2]
    zh, x, y = lax.axis_index("zh"), lax.axis_index("x"), lax.axis_index("y")
    zl, core = lax.axis_index("zl"), lax.axis_index("core")
    halves = (pl.ds(0, half), pl.ds(half, half))
    replica = zh * 4 + x
    shard = (y * 2 + zl) * 2 + core
    twin = (y * 2 + zl) * 2 + 1 - core

    def ring(i):
        return lax.rem(i + 1, 4), lax.rem(i + 3, 4), lax.rem(i + 2, 4)

    def lanes(i):
        return pl.ds(pl.multiple_of(i * cols, cols), cols)

    xn, zn, yn = ring(x), ring(zh), ring(y)
    yp, ym, yo = yn
    zl2, core2 = 1 - zl, 1 - core

    barrier = pltpu.get_barrier_semaphore()
    for peer in (
        {"x": xn[0]}, {"x": xn[1]}, {"zh": zn[0]}, {"zh": zn[1]},
        {"y": yp}, {"y": ym}, {"zl": zl2}, {"core": core2},
    ):
        pl.semaphore_signal(barrier, inc=1, device_id=peer, device_id_type=MESH)

    def load(c):
        for k in range(4):
            pltpu.make_async_copy(
                delta.at[c, :, pl.ds(k * 4 * cols, 4 * cols)], d.at[c, k], load_sem.at[c]
            ).start()

    for c in range(LA):
        load(c)
    if extra:
        for k in range(4):
            pltpu.make_async_copy(
                delta.at[pl.ds(nc, extra), :, pl.ds(k * 4 * cols, 4 * cols)],
                d.at[pl.ds(nc, extra), k], ex_sem,
            ).start()
    get_m = pltpu.make_async_copy(master, mst, mm_sem.at[0])
    get_v = pltpu.make_async_copy(momentum, mom, mm_sem.at[1])
    get_m.start()
    get_v.start()

    def load_next(c, carry):
        load(c)
        return carry

    lax.fori_loop(LA, nc, load_next, 0)

    count, twin_count = jnp.int32(0), jnp.int32(0)
    for b in range(own.shape[0]):
        count = count + (own[b] == shard).astype(jnp.int32)
        twin_count = twin_count + (own[b] == twin).astype(jnp.int32)

    def spare(c):
        i = c - per_block * count
        return i, (i >= 0) & (i < extra), jnp.clip(i, 0, max(extra - 1, 0))

    def is_live(c):
        i, inside, _ = spare(c)
        live = c < per_block * count
        if extra:
            live = live | (inside & (i + nc < per_block * twin_count))
        return live

    acc[...] = jnp.zeros_like(acc)
    pl.semaphore_wait(barrier, 8)

    def send(src, dst, ss, rs, peer):
        return pltpu.make_async_remote_copy(
            src_ref=src, dst_ref=dst, send_sem=ss, recv_sem=rs, device_id=peer, device_id_type=MESH
        )

    def xt_copy():
        return send(d.at[pl.ds(nc, extra)], xt, xt_sem.at[0], xt_sem.at[1], {"core": core2})

    def ax_copy():
        return send(axs, axr, ax_sem.at[0], ax_sem.at[1], {"core": core2})

    class Phase:
        def __init__(self, axis, near, slab, recv, sems):
            self.axis, self.near, self.slab = axis, near, slab
            self.r, self.dd, self.s = recv
            self.rs, self.rr, self.ds, self.dr, self.ss, self.sr = sems

        def relay(self, c, h):
            return send(
                self.slab(c, self.near[2], h), self.r.at[c, h],
                self.rs.at[c, h], self.rr.at[c, h], {self.axis: self.near[h]},
            )

        def direct(self, c, h):
            return send(
                self.slab(c, self.near[h], 1 - h), self.dd.at[c, h],
                self.ds.at[c, h], self.dr.at[c, h], {self.axis: self.near[h]},
            )

        def summed(self, c, h):
            return send(
                self.slab(c, self.near[h], h), self.s.at[c, h],
                self.ss.at[c, h], self.sr.at[c, h], {self.axis: self.near[h]},
            )

        def wait_sends(self, c):
            for f in (self.relay, self.direct, self.summed):
                for h in range(2):
                    f(c, h).wait_send()

    xph = Phase(
        "x", xn, lambda c, i, h: d.at[c, :, halves[h], lanes(i)],
        (xr, xd, xs), (xrs, xrr, xds, xdr, xss, xsr),
    )
    zph = Phase(
        "zh", zn, lambda c, i, h: d.at[c, i, halves[h], lanes(x)],
        (zr, zd, zs), (zrs, zrr, zds, zdr, zss, zsr),
    )

    def start_x(c, fixed=False):
        pltpu.make_async_copy(d.at[c], d.at[c], load_sem.at[c]).wait()
        if extra and not fixed:
            _, use, at = spare(c)

            @pl.when(c == per_block)
            def _():
                xt_copy().wait_recv()

            @pl.when(c >= per_block)
            def _():
                for k in range(4):
                    d[c, k] = jnp.where(use, xt[at, k], d[c, k])
        for h in range(2):
            xph.relay(c, h).start()
        for h in range(2):
            xph.direct(c, h).start()

    def sum_x(c):
        for h in range(2):
            xph.relay(c, h).wait_recv()
            for k in range(4):
                to = lanes(xn[h])
                d[c, k, halves[h], to] = (
                    d[c, k, halves[h], to].astype(F32) + xr[c, h, k].astype(F32)
                ).astype(BF16)
            xph.summed(c, h).start()

    def end_x(c):
        for h in range(2):
            xph.direct(c, h).wait_recv()
        for h in range(2):
            xph.summed(c, h).wait_recv()
        for h in range(2):
            for k in range(4):
                d[c, k, halves[h], lanes(x)] = (
                    d[c, k, halves[h], lanes(x)].astype(F32)
                    + xs[c, h, k].astype(F32)
                    + xd[c, 1 - h, k].astype(F32)
                ).astype(BF16)
        for h in range(2):
            zph.relay(c, h).start()
        for h in range(2):
            zph.direct(c, h).start()

    def sum_z(c):
        for h in range(2):
            zph.relay(c, h).wait_recv()
            to = zn[h]
            d[c, to, halves[h], lanes(x)] = (
                d[c, to, halves[h], lanes(x)].astype(F32) + zr[c, h].astype(F32)
            ).astype(BF16)
            zph.summed(c, h).start()

    def place(h, c):
        return h.at[:, :, core, pl.ds(pl.multiple_of(c * R, R), R), :]

    def g_copy(k, c, i):
        g = (ga, gb)[k]
        up, down = g.at[ym, :, c, halves[0], :], g.at[yp, :, c, halves[1], :]
        src = (
            g.at[y, zl, c], g.at[y, zl, c], g.at[y, zl, c],
            g.at[y, zl2, c], g.at[y, zl2, c], up, down, g.at[:, :, c],
        )[i]
        dst = place((ha, hb)[k], c) if i == 7 else src
        peer = (
            {"zl": zl2}, {"y": yp}, {"y": ym}, {"y": yp}, {"y": ym}, {"y": yp}, {"y": ym}, {"core": core2},
        )[i]
        return send(src, dst, gs.at[k, c, i], gr.at[k, c, i], peer)

    def g_local(k, c):
        return pltpu.make_async_copy((ga, gb)[k].at[:, :, c], place((ha, hb)[k], c), hs_sem.at[k, c])

    def g_start(k, c):
        for i in (0, 1, 2):
            g_copy(k, c, i).start()

    def g_second(k, c):
        g_copy(k, c, 0).wait_recv()
        for i in (3, 4):
            g_copy(k, c, i).start()

    def g_third(k, c):
        for i in (1, 2, 3, 4):
            g_copy(k, c, i).wait_recv()
        for i in (5, 6):
            g_copy(k, c, i).start()

    def g_last(k, c):
        for i in (5, 6):
            g_copy(k, c, i).wait_recv()
        g_copy(k, c, 7).start()
        g_local(k, c).start()

    def g_drain(k, c):
        for i in range(8):
            g_copy(k, c, i).wait_send()
        g_copy(k, c, 7).wait_recv()
        g_local(k, c).wait()

    def end_z(c):
        for h in range(2):
            zph.direct(c, h).wait_recv()
        for h in range(2):
            zph.summed(c, h).wait_recv()
        live = is_live(c)
        for h in range(2):
            value = (
                d[c, zh, halves[h], lanes(x)].astype(F32)
                + zs[c, h].astype(F32)
                + zd[c, 1 - h].astype(F32)
            ) * F32(0.0625)
            value = jnp.where(live, value, F32(0.0))
            gb[y, zl, c, halves[h], :] = value.astype(BF16)
            square = jnp.sum((value * value).reshape(half // 8, 8, cols), axis=0)
            part = square[:, :128]
            for k in range(1, cols // 128):
                part = part + square[:, k * 128:(k + 1) * 128]
            acc[...] += part
        g_start(1, c)

    def a_of(c, r):
        return (mst[c, r, :] - F32(0.567) * mom[c, r, :]).astype(BF16)

    def start_a(c, fixed=False):
        for r in halves:
            value = a_of(c, r)
            if extra and not fixed:
                _, use, at = spare(c)
                value = jnp.where(use, axr[at, r, :], value)
            ga[y, zl, c, r, :] = value
        g_start(0, c)

    def at(t, lag, f):
        @pl.when((t >= lag) & (t < nc + lag))
        def _():
            f(t - lag)

    def loop_body(t, carry):
        at(t, -LA, start_x)
        at(t, -LA, start_a)
        at(t, 0, sum_x)
        at(t, 1 - LA, functools.partial(g_second, 0))
        at(t, 1, end_x)
        at(t, 2 - LA, functools.partial(g_third, 0))
        at(t, 2, sum_z)
        at(t, 3, end_z)
        at(t, 3 - LA, functools.partial(g_last, 0))
        at(t, 4, functools.partial(g_second, 1))
        at(t, 5, functools.partial(g_third, 1))
        at(t, 6, functools.partial(g_last, 1))
        return carry

    def norm1(i):
        q = lax.rem(replica + i, 16)
        return send(
            n1.at[replica], n1.at[replica], n1s.at[i], n1r.at[i],
            {"zh": q // 4, "x": lax.rem(q, 4)},
        )

    def norm2(i):
        q = lax.rem(shard + i, 16)
        return send(
            n2.at[shard], n2.at[shard], n2s.at[i], n2r.at[i],
            {"y": q // 4, "zl": lax.rem(q // 2, 2), "core": lax.rem(q, 2)},
        )

    for c in range(LA):
        start_x(c, fixed=True)
    get_m.wait()
    get_v.wait()
    if extra:
        pltpu.make_async_copy(
            d.at[pl.ds(nc, extra)], d.at[pl.ds(nc, extra)], ex_sem
        ).wait()
        xt_copy().start()
        for e in range(extra):
            axs[e] = a_of(nc + e, slice(None))
        ax_copy().start()
    for c in range(LA):
        start_a(c, fixed=True)
    if extra:
        ax_copy().wait_recv()
    for t in range(1 - LA, 0):
        for lag, f in ((1, g_second), (2, g_third), (3, g_last)):
            if t - (lag - LA) >= 0:
                f(0, t - (lag - LA))
    lax.fori_loop(0, nc + 3, loop_body, 0)

    n1[replica] = jnp.sum(acc[...], axis=0, keepdims=True)
    for i in range(1, 16):
        norm1(i).start()
    g_second(1, nc - 1)
    g_third(1, nc - 2)
    g_last(1, nc - 3)

    def drain1(c, carry):
        xph.wait_sends(c)
        zph.wait_sends(c)
        return carry

    lax.fori_loop(0, nc, drain1, 0)
    if extra:
        xt_copy().wait_send()
        ax_copy().wait_send()
    g_third(1, nc - 1)
    g_last(1, nc - 2)
    for i in range(1, 16):
        norm1(i).wait_recv()
    n2[shard] = jnp.sum(n1[...], axis=0)
    for i in range(1, 16):
        norm2(i).start()

    def drain2(c, carry):
        g_drain(0, c)
        return carry

    def drain3(c, carry):
        g_drain(1, c)
        return carry

    g_last(1, nc - 1)
    lax.fori_loop(0, nc, drain2, 0)
    lax.fori_loop(0, nc - 2, drain3, 0)
    for i in range(1, 16):
        norm1(i).wait_send()
    for i in range(1, 16):
        norm2(i).wait_recv()
    tot[...] = jnp.sum(n2[...], axis=0)
    for i in range(1, 16):
        norm2(i).wait_send()
    lax.fori_loop(nc - 2, nc, drain3, 0)


def finish_kernel(
    own, size, tot, ha, hb, master, momentum,
    master_out, momentum_out, params,
    a, b, p, g, m, v, mo, vo, counts, slots, sem, gsem, msem, psem, osem,
):
    blocks = own.shape[0]
    per = params.shape[0] // blocks // HALF_BLOCK
    shard = (lax.axis_index("y") * 2 + lax.axis_index("zl")) * 2 + lax.axis_index("core")
    limit_of = SLOTS * per
    n = size[0]
    pltpu.make_async_copy(master, m, msem.at[0]).start()
    pltpu.make_async_copy(momentum, v, msem.at[1]).start()
    for k in range(16):
        counts[k] = 0
        slots[k] = 0
    for i in range(blocks):
        counts[own[i]] = counts[own[i]] + 1

    def flat(k, q):
        other = k + 1 - 2 * lax.rem(k, 2)
        return jnp.where(q < n, k * limit_of + q, other * limit_of + q - n + per * counts[other])

    def begin(i, carry):
        k = own[i]
        j = slots[k]
        slots[k] = j + 1
        for r in range(per):
            f = flat(k, j * per + r)
            pltpu.make_async_copy(ha.at[f], a.at[i, r], sem.at[0, i, r]).start()
            pltpu.make_async_copy(hb.at[f], b.at[i, r], sem.at[1, i, r]).start()
        return carry

    lax.fori_loop(0, blocks, begin, 0)
    count = counts[shard]
    for q in range(limit_of):
        f = jnp.where(q < per * count, flat(shard, q), 0)
        pltpu.make_async_copy(hb.at[f], g.at[q], gsem.at[q]).start()
    limit = 0.5 * jnp.sqrt(jnp.full((1, 1), params.shape[0] * params.shape[1] * 16, F32))
    total = jnp.sum(tot[...], axis=1, keepdims=True)
    factor = jnp.minimum(F32(1.0), limit / (jnp.sqrt(total) + F32(1e-06)))
    scale = F32(1.33) * factor

    def out(i):
        r = pl.ds(pl.multiple_of(i * BLOCK_ROWS, BLOCK_ROWS), BLOCK_ROWS)
        return pltpu.make_async_copy(p.at[i], params.at[r], psem.at[i])

    def block(i, carry):
        for r in range(per):
            pltpu.make_async_copy(ha.at[0], a.at[i, r], sem.at[0, i, r]).wait()
            pltpu.make_async_copy(hb.at[0], b.at[i, r], sem.at[1, i, r]).wait()
            for k in range(2):
                w = pl.ds(k * 32, 32)
                p[i, pl.ds(r * HALF_BLOCK + k * 32, 32), :] = (
                    a[i, r, w, :].astype(F32) - scale * b[i, r, w, :].astype(F32)
                ).astype(BF16)
        out(i).start()
        return carry

    lax.fori_loop(0, blocks, block, 0)
    pltpu.make_async_copy(master, m, msem.at[0]).wait()
    pltpu.make_async_copy(momentum, v, msem.at[1]).wait()

    def update(q, carry):
        pltpu.make_async_copy(hb.at[0], g.at[q], gsem.at[q]).wait()
        live = q < per * count
        for k in range(2):
            w = pl.ds(k * 32, 32)
            r = pl.ds(pl.multiple_of(q * HALF_BLOCK + k * 32, 32), 32)
            grad = factor * g[q, w, :].astype(F32)
            old = v[r, :]
            new = jnp.where(live, F32(0.9) * old + grad, old)
            z = m[r, :]
            vo[r, :] = new
            mo[r, :] = jnp.where(live, z - F32(0.7) * (grad + F32(0.9) * new), z)
        return carry

    lax.fori_loop(0, limit_of, update, 0)
    put_m = pltpu.make_async_copy(mo, master_out, osem.at[0])
    put_v = pltpu.make_async_copy(vo, momentum_out, osem.at[1])
    put_m.start()
    put_v.start()

    def end(i, carry):
        out(i).wait()
        return carry

    lax.fori_loop(0, blocks, end, 0)
    put_m.wait()
    put_v.wait()


def size_kernel(own, size):
    chips = [jnp.int32(0)] * 8
    for i in range(own.shape[0]):
        chip = own[i] // 2
        chips = [n + (chip == k).astype(jnp.int32) for k, n in enumerate(chips)]
    most = functools.reduce(jnp.maximum, chips)
    size[0] = jnp.maximum(most, SIZES[0])


SIZES = (5, 6, 7, 8)


def on_device(deltas, master, momentum, block_owner):
    rows, cols = master.shape
    width = deltas.shape[2]
    chunks = rows // R
    half = R // 2
    own = block_owner.reshape(-1)
    blocks = own.shape[0]
    any_spec = pl.BlockSpec(memory_space=pl.ANY)
    vmem = pl.BlockSpec(memory_space=pltpu.VMEM)
    smem = pl.BlockSpec(memory_space=pltpu.SMEM)
    sem = pltpu.SemaphoreType.DMA
    gathered = jax.ShapeDtypeStruct((4, 2, 2, rows, cols), BF16)

    def comm(size, ident):
        nc = size * HALF_BLOCK // R
        extra = max(chunks - nc, 1)
        call = pl.pallas_call(
            functools.partial(comm_kernel, nc),
            name=f"reduce_gather_{size}",
            out_shape=(gathered, gathered, jax.ShapeDtypeStruct((1, 128), F32)),
            in_specs=[smem, any_spec, any_spec, any_spec],
            out_specs=(any_spec, any_spec, vmem),
            scratch_shapes=(
                [pltpu.VMEM((chunks, 4, R, 4 * cols), BF16)]
                + [pltpu.VMEM((extra, 4, R, 4 * cols), BF16)]
                + [pltpu.VMEM((nc, 2, 4, half, cols), BF16)] * 3
                + [pltpu.VMEM((nc, 2, half, cols), BF16)] * 3
                + [pltpu.VMEM((4, 2, nc, R, cols), BF16)] * 2
                + [pltpu.VMEM((chunks, R, cols), F32)] * 2
                + [pltpu.VMEM((extra, R, cols), BF16)] * 2
                + [pltpu.VMEM((8, 128), F32)]
                + [pltpu.VMEM((16, 1, 128), F32)] * 2
                + [sem((nc,)), sem, sem((2,)), sem((2,)), sem((2,))]
                + [sem((nc, 2))] * 12
                + [sem((2, nc, 8))] * 2
                + [sem((2, nc))]
                + [sem((16,))] * 4
            ),
            compiler_params=pltpu.CompilerParams(
                collective_id=ident, has_side_effects=True, vmem_limit_bytes=60 * 1024 * 1024
            ),
        )
        return lambda o, d, m, v: call(o, d, m, v)

    size = pl.pallas_call(
        size_kernel,
        name="size",
        out_shape=jax.ShapeDtypeStruct((1,), jnp.int32),
        in_specs=[smem],
        out_specs=smem,
    )(own)
    operands = (
        own,
        deltas.reshape(chunks, R, width),
        master.reshape(chunks, R, cols),
        momentum.reshape(chunks, R, cols),
    )
    branches = [comm(s, i) for i, s in enumerate(SIZES)]
    if len(branches) == 1:
        ha, hb, tot = branches[0](*operands)
    else:
        ha, hb, tot = lax.switch(size[0] - SIZES[0], branches, *operands)
    parts = 16 * rows // HALF_BLOCK
    ha = ha.reshape(parts, HALF_BLOCK, cols)
    hb = hb.reshape(parts, HALF_BLOCK, cols)
    per = BLOCK_ROWS // HALF_BLOCK
    return pl.pallas_call(
        finish_kernel,
        name="finish",
        out_shape=(
            jax.ShapeDtypeStruct((rows, cols), F32),
            jax.ShapeDtypeStruct((rows, cols), F32),
            jax.ShapeDtypeStruct((blocks * BLOCK_ROWS, cols), BF16),
        ),
        in_specs=[smem, smem, vmem] + [any_spec] * 4,
        out_specs=(any_spec, any_spec, any_spec),
        scratch_shapes=(
            [pltpu.VMEM((blocks, per, HALF_BLOCK, cols), BF16)] * 2
            + [pltpu.VMEM((blocks, BLOCK_ROWS, cols), BF16)]
            + [pltpu.VMEM((SLOTS * per, HALF_BLOCK, cols), BF16)]
            + [pltpu.VMEM((rows, cols), F32)] * 4
            + [pltpu.SMEM((16,), jnp.int32)] * 2
            + [sem((2, blocks, per)), sem((SLOTS * per,)), sem((2,)), sem((blocks,)), sem((2,))]
        ),
        compiler_params=pltpu.CompilerParams(vmem_limit_bytes=60 * 1024 * 1024),
    )(own, size, tot, ha, hb, master, momentum)


def solution(mesh):
    finer = Mesh(mesh.devices.reshape(4, 4, 4, 2, 2), AXES)
    replica, shard = AXES[:2], AXES[2:]
    in_specs = (P(replica, shard, None), P(shard, replica), P(shard, replica), P())
    out_specs = (P(shard, replica), P(shard, replica), P(None, replica))
    return jax.shard_map(
        on_device, mesh=finer, in_specs=in_specs, out_specs=out_specs, check_vma=False
    )
```

```python
import functools

import jax
import jax.numpy as jnp
from jax import lax
from jax.experimental import pallas as pl
from jax.experimental.pallas import tpu as pltpu
from jax.sharding import Mesh
from jax.sharding import PartitionSpec as P

BLOCK_ROWS = 128
SLOTS = 4
HALF_BLOCK = 64
AXES = ("zh", "x", "y", "zl", "core")
MESH = pl.DeviceIdType.MESH
R = 32
DIRECT = 1
F32 = jnp.float32
BF16 = jnp.bfloat16


def comm_kernel(
    nc,
    own, delta, master, momentum,
    ha, hb, tot,
    d, xt, xr, xe, zr, ze, zf, mst, mom, axs, axr, acc, n1, n2,
    load_sem, ex_sem, mm_sem, xt_sem, ax_sem,
    xrr, xer, zrr, zer, zf_sem, send_sem,
    gr0, gr1, gr2, gr3, gs, n_sem,
):
    chunks = d.shape[0]
    extra = chunks - nc
    per_block = BLOCK_ROWS // R
    half = R // 2
    cols = master.shape[2]
    zh, x, y = lax.axis_index("zh"), lax.axis_index("x"), lax.axis_index("y")
    zl, core = lax.axis_index("zl"), lax.axis_index("core")
    halves = (pl.ds(0, half), pl.ds(half, half))
    replica = zh * 4 + x
    shard = (y * 2 + zl) * 2 + core
    twin = (y * 2 + zl) * 2 + 1 - core

    def ring(i):
        return lax.rem(i + 1, 4), lax.rem(i + 3, 4), lax.rem(i + 2, 4)

    def lanes(i):
        return pl.ds(pl.multiple_of(i * cols, cols), cols)

    xn, zn, yn = ring(x), ring(zh), ring(y)
    yp, ym, yo = yn
    zl2, core2 = 1 - zl, 1 - core

    barrier = pltpu.get_barrier_semaphore()
    for peer in (
        {"x": xn[0]}, {"x": xn[1]}, {"zh": zn[0]}, {"zh": zn[1]},
        {"y": yp}, {"y": ym}, {"zl": zl2}, {"core": core2},
    ):
        pl.semaphore_signal(barrier, inc=1, device_id=peer, device_id_type=MESH)

    def load(c):
        for k in range(4):
            pltpu.make_async_copy(
                delta.at[c, :, pl.ds(k * 4 * cols, 4 * cols)], d.at[c, k], load_sem.at[c]
            ).start()

    load(0)
    load(1)
    get_m = pltpu.make_async_copy(master, mst, mm_sem.at[0])
    get_v = pltpu.make_async_copy(momentum, mom, mm_sem.at[1])
    get_m.start()
    get_v.start()
    if extra:
        for k in range(4):
            pltpu.make_async_copy(
                delta.at[pl.ds(nc, extra), :, pl.ds(k * 4 * cols, 4 * cols)],
                d.at[pl.ds(nc, extra), k], ex_sem,
            ).start()

    def load_next(c, carry):
        load(c)
        return carry

    lax.fori_loop(2, nc, load_next, 0)

    count, twin_count = jnp.int32(0), jnp.int32(0)
    for b in range(own.shape[0]):
        count = count + (own[b] == shard).astype(jnp.int32)
        twin_count = twin_count + (own[b] == twin).astype(jnp.int32)

    def spare(c):
        i = c - per_block * count
        return i, (i >= 0) & (i < extra), jnp.clip(i, 0, max(extra - 1, 0))

    def is_live(c):
        i, inside, _ = spare(c)
        live = c < per_block * count
        if extra:
            live = live | (inside & (i + nc < per_block * twin_count))
        return live

    acc[...] = jnp.zeros_like(acc)
    pl.semaphore_wait(barrier, 8)

    def send(src, dst, ss, rs, peer):
        return pltpu.make_async_remote_copy(
            src_ref=src, dst_ref=dst, send_sem=ss, recv_sem=rs, device_id=peer, device_id_type=MESH
        )

    def xt_copy():
        return send(d.at[pl.ds(nc, extra)], xt, xt_sem.at[0], xt_sem.at[1], {"core": core2})

    def ax_copy():
        return send(axs, axr, ax_sem.at[0], ax_sem.at[1], {"core": core2})

    def wait_for(ref, sem):
        pltpu.make_async_copy(ref, ref, sem).wait()

    class Phase:
        def __init__(self, axis, near, slab, r, e, rr, er, first):
            self.axis, self.near, self.slab = axis, near, slab
            self.r, self.e, self.rr, self.er, self.first = r, e, rr, er, first

        def relay(self, c, h):
            return send(
                self.slab(c, self.near[2], h), self.r.at[c, h],
                send_sem.at[self.first], self.rr.at[c], {self.axis: self.near[h]},
            )

        def direct(self, c, h):
            return send(
                self.slab(c, self.near[h], 1 - h), self.e.at[c, 0, h],
                send_sem.at[self.first + 1], self.er.at[c], {self.axis: self.near[h]},
            )

        def summed(self, c, h):
            return send(
                self.slab(c, self.near[h], h), self.e.at[c, 1, h],
                send_sem.at[self.first + 2], self.er.at[c], {self.axis: self.near[h]},
            )

        def wait_relay(self, c):
            wait_for(self.r.at[c], self.rr.at[c])

        def wait_sends(self):
            for i, ref in enumerate((self.r, self.e.at[:, 0], self.e.at[:, 1])):
                wait_for(ref, send_sem.at[self.first + i])

    xph = Phase("x", xn, lambda c, i, h: d.at[c, :, halves[h], lanes(i)], xr, xe, xrr, xer, 0)
    zph = Phase("zh", zn, lambda c, i, h: d.at[c, i, halves[h], lanes(x)], zr, ze, zrr, zer, 3)

    def start_x(c, fixed=False):
        pltpu.make_async_copy(d.at[c], d.at[c], load_sem.at[c]).wait()
        if extra and not fixed:
            _, use, at = spare(c)

            @pl.when(c == per_block)
            def _():
                xt_copy().wait_recv()

            @pl.when(c >= per_block)
            def _():
                for k in range(4):
                    d[c, k] = jnp.where(use, xt[at, k], d[c, k])
        for h in range(2):
            xph.relay(c, h).start()
        for h in range(2):
            xph.direct(c, h).start()

    def sum_x(c):
        xph.wait_relay(c)
        for h in range(2):
            for k in range(4):
                to = lanes(xn[h])
                d[c, k, halves[h], to] = (
                    d[c, k, halves[h], to].astype(F32) + xr[c, h, k].astype(F32)
                ).astype(BF16)
            xph.summed(c, h).start()

    def z_full(k, j):
        return send(
            d.at[nc - DIRECT + k, zn[j], :, lanes(x)], zf.at[k, j],
            zf_sem.at[0], zf_sem.at[1 + k], {"zh": zn[j]},
        )

    def end_x(c, final=None):
        wait_for(xe.at[c], xer.at[c])
        for h in range(2):
            for k in range(4):
                d[c, k, halves[h], lanes(x)] = (
                    d[c, k, halves[h], lanes(x)].astype(F32)
                    + xe[c, 1, h, k].astype(F32)
                    + xe[c, 0, 1 - h, k].astype(F32)
                ).astype(BF16)
        if final is not None:
            for j in (2, 0, 1):
                z_full(final, j).start()
            return
        for h in range(2):
            zph.relay(c, h).start()
        for h in range(2):
            zph.direct(c, h).start()

    def sum_z(c):
        zph.wait_relay(c)
        for h in range(2):
            to = zn[h]
            d[c, to, halves[h], lanes(x)] = (
                d[c, to, halves[h], lanes(x)].astype(F32) + zr[c, h].astype(F32)
            ).astype(BF16)
            zph.summed(c, h).start()

    def g_copy(k, c, i):
        g = (ha, hb)[k]
        mine_at, other_at = g.at[y, zl, core, c], g.at[y, zl2, core, c]
        up, down = g.at[ym, :, core, c, halves[0], :], g.at[yp, :, core, c, halves[1], :]
        ref = (mine_at, mine_at, mine_at, other_at, other_at, up, down, g.at[:, :, core, c])[i]
        peer = (
            {"zl": zl2}, {"y": yp}, {"y": ym}, {"y": yp}, {"y": ym}, {"y": yp}, {"y": ym}, {"core": core2},
        )[i]
        arrive = (gr0, gr1, gr1, gr1, gr1, gr2, gr2)[i].at[k, c] if i < 7 else gr3.at[k]
        return send(ref, ref, gs.at[k, i], arrive, peer)

    def g_start(k, c):
        for i in (0, 1, 2):
            g_copy(k, c, i).start()

    def g_second(k, c):
        g_copy(k, c, 0).wait_recv()
        for i in (3, 4):
            g_copy(k, c, i).start()

    def g_third(k, c):
        wait_for((ha, hb)[k].at[0, 0, 0, pl.ds(0, 4)], gr1.at[k, c])
        for i in (5, 6):
            g_copy(k, c, i).start()

    def g_last(k, c):
        wait_for((ha, hb)[k].at[0, 0, 0, pl.ds(0, 2)], gr2.at[k, c])
        g_copy(k, c, 7).start()

    def g_drain(k):
        g = (ha, hb)[k]
        for i in range(7):
            wait_for(g.at[0, 0, 0, pl.ds(0, nc)], gs.at[k, i])
        for arrive in (gs.at[k, 7], gr3.at[k]):
            wait_for(g.at[:, :, 0, pl.ds(0, nc)], arrive)

    def end_z(c, final=None):
        if final is not None:
            wait_for(zf.at[final], zf_sem.at[1 + final])
        else:
            wait_for(ze.at[c], zer.at[c])
        live = is_live(c)
        for h in range(2):
            value = d[c, zh, halves[h], lanes(x)].astype(F32)
            if final is not None:
                parts = [zf[final, j, halves[h], :] for j in range(3)]
            else:
                parts = [ze[c, 1, h], ze[c, 0, 1 - h]]
            for part in parts:
                value = value + part.astype(F32)
            value = value * F32(0.0625)
            value = jnp.where(live, value, F32(0.0))
            hb[y, zl, core, c, halves[h], :] = value.astype(BF16)
            square = jnp.sum((value * value).reshape(half // 8, 8, cols), axis=0)
            part = square[:, :128]
            for k in range(1, cols // 128):
                part = part + square[:, k * 128:(k + 1) * 128]
            acc[...] += part
        g_start(1, c)

    def a_of(c, r):
        return (mst[c, r, :] - F32(0.567) * mom[c, r, :]).astype(BF16)

    def start_a(c, fixed=False):
        if extra and not fixed:

            @pl.when(c == per_block)
            def _():
                ax_copy().wait_recv()

        for r in halves:
            ha[y, zl, core, c, r, :] = a_of(c, r)
        if extra and not fixed:
            _, use, spot = spare(c)

            @pl.when(c >= per_block)
            def _():
                for r in halves:
                    value = ha[y, zl, core, c, r, :]
                    ha[y, zl, core, c, r, :] = jnp.where(use, axr[spot, r, :], value)
        g_start(0, c)

    def at(t, lag, f):
        @pl.when((t >= lag) & (t < nc + lag))
        def _():
            f(t - lag)

    def pair(t, lag, f):
        @pl.when((t >= lag) & (t < nc // 2 + lag))
        def _():
            f(2 * (t - lag))
            f(2 * (t - lag) + 1)

    second = [functools.partial(g_second, k) for k in range(2)]
    third = [functools.partial(g_third, k) for k in range(2)]
    last = [functools.partial(g_last, k) for k in range(2)]

    def loop_body(t, carry):
        @pl.when((t >= 1) & (t < nc - 1))
        def _():
            start_x(t + 1)

        pair(t, -1, start_a)
        at(t, 0, sum_x)
        pair(t, 0, second[0])
        at(t, 1, end_x)
        pair(t, 1, third[0])
        at(t, 2, sum_z)
        at(t, 3, end_z)
        pair(t, 2, last[0])
        at(t, 4, second[1])
        at(t, 5, third[1])
        at(t, 6, last[1])
        return carry

    def direct(c):
        return c - (nc - DIRECT) if c >= nc - DIRECT else None

    def norm1(i):
        q = lax.rem(replica + i, 16)
        return send(
            n1.at[replica], n1.at[replica], n_sem.at[0], n_sem.at[1],
            {"zh": q // 4, "x": lax.rem(q, 4)},
        )

    def norm2(i):
        q = lax.rem(shard + i, 16)
        return send(
            n2.at[shard], n2.at[shard], n_sem.at[2], n_sem.at[3],
            {"y": q // 4, "zl": lax.rem(q // 2, 2), "core": lax.rem(q, 2)},
        )

    start_x(0, fixed=True)
    start_x(1, fixed=True)
    get_m.wait()
    get_v.wait()
    start_a(0, fixed=True)
    start_a(1, fixed=True)
    if extra:
        wait_for(d.at[pl.ds(nc, extra)], ex_sem)
        xt_copy().start()
        for e in range(extra):
            axs[e] = a_of(nc + e, slice(None))
        ax_copy().start()
    lax.fori_loop(0, nc - 1, loop_body, 0)

    n = nc
    sum_x(n - 1)
    end_x(n - 2, final=direct(n - 2))
    sum_z(n - 3)
    end_z(n - 4)
    second[1](n - 5)
    third[1](n - 6)
    last[1](n - 7)
    end_x(n - 1, final=direct(n - 1))
    if direct(n - 2) is None:
        sum_z(n - 2)
    second[1](n - 4)
    end_z(n - 3)
    if direct(n - 1) is None:
        sum_z(n - 1)
    third[1](n - 5)
    last[1](n - 6)
    end_z(n - 2, final=direct(n - 2))
    end_z(n - 1, final=direct(n - 1))
    n1[replica] = jnp.sum(acc[...], axis=0, keepdims=True)
    for i in range(1, 16):
        norm1(i).start()
    second[1](n - 3)
    third[1](n - 4)
    second[1](n - 2)
    last[1](n - 5)
    second[1](n - 1)
    third[1](n - 3)
    last[1](n - 4)
    third[1](n - 2)
    xph.wait_sends()
    zph.wait_sends()
    if extra:
        xt_copy().wait_send()
        ax_copy().wait_send()
    last[1](n - 3)
    third[1](n - 1)
    some = pl.ds(0, 15)
    wait_for(n1.at[some], n_sem.at[1])
    n2[shard] = jnp.sum(n1[...], axis=0)
    for i in range(1, 16):
        norm2(i).start()
    last[1](n - 2)
    last[1](n - 1)
    g_drain(0)
    if DIRECT:
        wait_for(zf, zf_sem.at[0])
    wait_for(n1.at[some], n_sem.at[0])
    wait_for(n2.at[some], n_sem.at[3])
    tot[...] = jnp.sum(n2[...], axis=0)
    wait_for(n2.at[some], n_sem.at[2])
    g_drain(1)


def finish_kernel(
    own, size, tot, ha, hb, master, momentum,
    master_out, momentum_out, params,
    p, m, v, mo, vo, counts, slots, in_sem, out_sem,
):
    blocks = own.shape[0]
    per = params.shape[0] // blocks // HALF_BLOCK
    limit_of = SLOTS * per
    shard = (lax.axis_index("y") * 2 + lax.axis_index("zl")) * 2 + lax.axis_index("core")
    n = size[0]
    get_m = pltpu.make_async_copy(master, m, in_sem.at[0])
    get_v = pltpu.make_async_copy(momentum, v, in_sem.at[1])
    get_m.start()
    get_v.start()
    for k in range(16):
        counts[k] = 0
        slots[k] = 0
    for i in range(blocks):
        counts[own[i]] = counts[own[i]] + 1

    def flat(k, q):
        other = k + 1 - 2 * lax.rem(k, 2)
        return jnp.where(q < n, k * limit_of + q, other * limit_of + q - n + per * counts[other])

    limit = 0.5 * jnp.sqrt(jnp.full((1, 1), params.shape[0] * params.shape[1] * 16, F32))
    total = jnp.sum(tot[...], axis=1, keepdims=True)
    factor = jnp.minimum(F32(1.0), limit / (jnp.sqrt(total) + F32(1e-06)))
    scale = F32(1.33) * factor

    def block(i, carry):
        k = own[i]
        j = slots[k]
        slots[k] = j + 1
        for r in range(per):
            f = flat(k, j * per + r)
            for h in range(2):
                w = pl.ds(h * 32, 32)
                p[i, pl.ds(r * HALF_BLOCK + h * 32, 32), :] = (
                    ha[f, w, :].astype(F32) - scale * hb[f, w, :].astype(F32)
                ).astype(BF16)
        rows = pl.ds(pl.multiple_of(i * BLOCK_ROWS, BLOCK_ROWS), BLOCK_ROWS)
        pltpu.make_async_copy(p.at[i], params.at[rows], out_sem.at[2]).start()
        return carry

    lax.fori_loop(0, 8, block, 0)
    get_m.wait()
    get_v.wait()
    count = counts[shard]

    def update(q, carry):
        live = q < per * count
        f = jnp.where(live, flat(shard, q), 0)
        for h in range(2):
            r = pl.ds(pl.multiple_of(q * HALF_BLOCK + h * 32, 32), 32)
            grad = factor * hb[f, pl.ds(h * 32, 32), :].astype(F32)
            old = v[r, :]
            new = jnp.where(live, F32(0.9) * old + grad, old)
            z = m[r, :]
            vo[r, :] = new
            mo[r, :] = jnp.where(live, z - F32(0.7) * (grad + F32(0.9) * new), z)
        return carry

    lax.fori_loop(0, limit_of, update, 0)
    put_m = pltpu.make_async_copy(mo, master_out, out_sem.at[0])
    put_v = pltpu.make_async_copy(vo, momentum_out, out_sem.at[1])
    put_m.start()
    put_v.start()
    lax.fori_loop(8, blocks, block, 0)
    put_m.wait()
    put_v.wait()
    pltpu.make_async_copy(p, p, out_sem.at[2]).wait()


def size_kernel(own, size):
    chips = [jnp.int32(0)] * 8
    for i in range(own.shape[0]):
        chip = own[i] // 2
        chips = [n + (chip == k).astype(jnp.int32) for k, n in enumerate(chips)]
    most = functools.reduce(jnp.maximum, chips)
    size[0] = jnp.maximum(most, SIZES[0])


SIZES = (5, 6, 7, 8)


def on_device(deltas, master, momentum, block_owner):
    rows, cols = master.shape
    width = deltas.shape[2]
    chunks = rows // R
    half = R // 2
    own = block_owner.reshape(-1)
    blocks = own.shape[0]
    any_spec = pl.BlockSpec(memory_space=pl.ANY)
    vmem = pl.BlockSpec(memory_space=pltpu.VMEM)
    smem = pl.BlockSpec(memory_space=pltpu.SMEM)
    sem = pltpu.SemaphoreType.DMA
    gathered = jax.ShapeDtypeStruct((4, 2, 2, chunks, R, cols), BF16)

    def comm(size, ident):
        nc = size * HALF_BLOCK // R
        extra = max(chunks - nc, 1)
        call = pl.pallas_call(
            functools.partial(comm_kernel, nc),
            name=f"reduce_gather_{size}",
            out_shape=(gathered, gathered, jax.ShapeDtypeStruct((1, 128), F32)),
            in_specs=[smem, any_spec, any_spec, any_spec],
            out_specs=(vmem, vmem, vmem),
            scratch_shapes=(
                [pltpu.VMEM((chunks, 4, R, 4 * cols), BF16)]
                + [pltpu.VMEM((extra, 4, R, 4 * cols), BF16)]
                + [pltpu.VMEM((nc, 2, 4, half, cols), BF16)]
                + [pltpu.VMEM((nc, 2, 2, 4, half, cols), BF16)]
                + [pltpu.VMEM((nc - DIRECT, 2, half, cols), BF16)]
                + [pltpu.VMEM((nc - DIRECT, 2, 2, half, cols), BF16)]
                + [pltpu.VMEM((max(DIRECT, 1), 3, R, cols), BF16)]
                + [pltpu.VMEM((chunks, R, cols), F32)] * 2
                + [pltpu.VMEM((extra, R, cols), BF16)] * 2
                + [pltpu.VMEM((8, 128), F32)]
                + [pltpu.VMEM((16, 1, 128), F32)] * 2
                + [sem((nc,)), sem, sem((2,)), sem((2,)), sem((2,))]
                + [sem((nc,))] * 2
                + [sem((nc - DIRECT,))] * 2
                + [sem((1 + DIRECT,)), sem((6,))]
                + [sem((2, nc))] * 3
                + [sem((2,)), sem((2, 8)), sem((4,))]
            ),
            compiler_params=pltpu.CompilerParams(
                collective_id=ident, has_side_effects=True, vmem_limit_bytes=30 * 1024 * 1024
            ),
        )
        return lambda o, d, m, v: call(o, d, m, v)

    size = pl.pallas_call(
        size_kernel,
        name="size",
        out_shape=jax.ShapeDtypeStruct((1,), jnp.int32),
        in_specs=[smem],
        out_specs=smem,
    )(own)
    operands = (
        own,
        deltas.reshape(chunks, R, width),
        master.reshape(chunks, R, cols),
        momentum.reshape(chunks, R, cols),
    )
    branches = [comm(s, i) for i, s in enumerate(SIZES)]
    if len(branches) == 1:
        ha, hb, tot = branches[0](*operands)
    else:
        ha, hb, tot = lax.switch(size[0] - SIZES[0], branches, *operands)
    parts = 16 * rows // HALF_BLOCK
    ha = ha.reshape(parts, HALF_BLOCK, cols)
    hb = hb.reshape(parts, HALF_BLOCK, cols)
    return pl.pallas_call(
        finish_kernel,
        name="finish",
        out_shape=(
            jax.ShapeDtypeStruct((rows, cols), F32),
            jax.ShapeDtypeStruct((rows, cols), F32),
            jax.ShapeDtypeStruct((blocks * BLOCK_ROWS, cols), BF16),
        ),
        in_specs=[smem, smem, vmem, vmem, vmem] + [any_spec] * 2,
        out_specs=(any_spec, any_spec, any_spec),
        scratch_shapes=(
            [pltpu.VMEM((blocks, BLOCK_ROWS, cols), BF16)]
            + [pltpu.VMEM((rows, cols), F32)] * 4
            + [pltpu.SMEM((16,), jnp.int32)] * 2
            + [sem((2,)), sem((3,))]
        ),
        compiler_params=pltpu.CompilerParams(vmem_limit_bytes=12 * 1024 * 1024),
    )(own, size, tot, ha, hb, master, momentum)


def solution(mesh):
    finer = Mesh(mesh.devices.reshape(4, 4, 4, 2, 2), AXES)
    replica, shard = AXES[:2], AXES[2:]
    in_specs = (P(replica, shard, None), P(shard, replica), P(shard, replica), P())
    out_specs = (P(shard, replica), P(shard, replica), P(None, replica))
    return jax.shard_map(
        on_device, mesh=finer, in_specs=in_specs, out_specs=out_specs, check_vma=False
    )
```

```python
import functools

import jax
import jax.numpy as jnp
from jax import lax
from jax.experimental import pallas as pl
from jax.experimental.pallas import tpu as pltpu
from jax.sharding import Mesh
from jax.sharding import PartitionSpec as P

BLOCK_ROWS = 128
SLOTS = 4
HALF_BLOCK = 64
AXES = ("zh", "x", "y", "zl", "core")
MESH = pl.DeviceIdType.MESH
R = 32
DIRECT = 1
F32 = jnp.float32
BF16 = jnp.bfloat16


def comm_kernel(
    nc,
    own, delta, master, momentum,
    ha, hb, tot,
    d, xt, xr, xe, zr, ze, zf, mst, mom, axs, axr, acc, n1, n2,
    load_sem, ex_sem, mm_sem, xt_sem, ax_sem,
    xrr, xer, zrr, zer, zf_sem, send_sem,
    gr0, gr1, gr2, gr3, gs, n_sem,
):
    chunks = d.shape[0]
    extra = chunks - nc
    per_block = BLOCK_ROWS // R
    half = R // 2
    cols = master.shape[2]
    zh, x, y = lax.axis_index("zh"), lax.axis_index("x"), lax.axis_index("y")
    zl, core = lax.axis_index("zl"), lax.axis_index("core")
    halves = (pl.ds(0, half), pl.ds(half, half))
    replica = zh * 4 + x
    shard = (y * 2 + zl) * 2 + core
    twin = (y * 2 + zl) * 2 + 1 - core

    def ring(i):
        return lax.rem(i + 1, 4), lax.rem(i + 3, 4), lax.rem(i + 2, 4)

    def lanes(i):
        return pl.ds(pl.multiple_of(i * cols, cols), cols)

    xn, zn, yn = ring(x), ring(zh), ring(y)
    yp, ym, yo = yn
    zl2, core2 = 1 - zl, 1 - core

    barrier = pltpu.get_barrier_semaphore()
    for peer in (
        {"x": xn[0]}, {"x": xn[1]}, {"zh": zn[0]}, {"zh": zn[1]},
        {"y": yp}, {"y": ym}, {"zl": zl2}, {"core": core2},
    ):
        pl.semaphore_signal(barrier, inc=1, device_id=peer, device_id_type=MESH)

    def load(c):
        for k in range(4):
            pltpu.make_async_copy(
                delta.at[c, :, pl.ds(k * 4 * cols, 4 * cols)], d.at[c, k], load_sem.at[c]
            ).start()

    load(0)
    load(1)
    get_m = pltpu.make_async_copy(master, mst, mm_sem.at[0])
    get_v = pltpu.make_async_copy(momentum, mom, mm_sem.at[1])
    get_m.start()
    get_v.start()
    if extra:
        for k in range(4):
            pltpu.make_async_copy(
                delta.at[pl.ds(nc, extra), :, pl.ds(k * 4 * cols, 4 * cols)],
                d.at[pl.ds(nc, extra), k], ex_sem,
            ).start()

    def load_next(c, carry):
        load(c)
        return carry

    lax.fori_loop(2, nc, load_next, 0)

    count, twin_count = jnp.int32(0), jnp.int32(0)
    for b in range(own.shape[0]):
        count = count + (own[b] == shard).astype(jnp.int32)
        twin_count = twin_count + (own[b] == twin).astype(jnp.int32)

    def spare(c):
        i = c - per_block * count
        return i, (i >= 0) & (i < extra), jnp.clip(i, 0, max(extra - 1, 0))

    def is_live(c):
        i, inside, _ = spare(c)
        live = c < per_block * count
        if extra:
            live = live | (inside & (i + nc < per_block * twin_count))
        return live

    acc[...] = jnp.zeros_like(acc)
    pl.semaphore_wait(barrier, 8)

    def send(src, dst, ss, rs, peer):
        return pltpu.make_async_remote_copy(
            src_ref=src, dst_ref=dst, send_sem=ss, recv_sem=rs, device_id=peer, device_id_type=MESH
        )

    def xt_copy():
        return send(d.at[pl.ds(nc, extra)], xt, xt_sem.at[0], xt_sem.at[1], {"core": core2})

    def ax_copy():
        return send(axs, axr, ax_sem.at[0], ax_sem.at[1], {"core": core2})

    def wait_for(ref, sem):
        pltpu.make_async_copy(ref, ref, sem).wait()

    class Phase:
        def __init__(self, axis, near, slab, r, e, rr, er, first):
            self.axis, self.near, self.slab = axis, near, slab
            self.r, self.e, self.rr, self.er, self.first = r, e, rr, er, first

        def relay(self, c, h):
            return send(
                self.slab(c, self.near[2], h), self.r.at[c, h],
                send_sem.at[self.first], self.rr.at[c], {self.axis: self.near[h]},
            )

        def direct(self, c, h):
            return send(
                self.slab(c, self.near[h], 1 - h), self.e.at[c, 0, h],
                send_sem.at[self.first + 1], self.er.at[c], {self.axis: self.near[h]},
            )

        def summed(self, c, h):
            return send(
                self.slab(c, self.near[h], h), self.e.at[c, 1, h],
                send_sem.at[self.first + 2], self.er.at[c], {self.axis: self.near[h]},
            )

        def wait_relay(self, c):
            wait_for(self.r.at[c], self.rr.at[c])

        def wait_sends(self):
            for i, ref in enumerate((self.r, self.e.at[:, 0], self.e.at[:, 1])):
                wait_for(ref, send_sem.at[self.first + i])

    xph = Phase("x", xn, lambda c, i, h: d.at[c, :, halves[h], lanes(i)], xr, xe, xrr, xer, 0)
    zph = Phase("zh", zn, lambda c, i, h: d.at[c, i, halves[h], lanes(x)], zr, ze, zrr, zer, 3)

    def start_x(c, fixed=False):
        pltpu.make_async_copy(d.at[c], d.at[c], load_sem.at[c]).wait()
        if extra and not fixed:
            _, use, at = spare(c)

            @pl.when(c == per_block)
            def _():
                xt_copy().wait_recv()

            @pl.when(c >= per_block)
            def _():
                for k in range(4):
                    d[c, k] = jnp.where(use, xt[at, k], d[c, k])
        for h in range(2):
            xph.relay(c, h).start()

    def direct_x(c):
        for h in range(2):
            xph.direct(c, h).start()

    def sum_x(c):
        xph.wait_relay(c)
        for h in range(2):
            for k in range(4):
                to = lanes(xn[h])
                d[c, k, halves[h], to] = (
                    d[c, k, halves[h], to].astype(F32) + xr[c, h, k].astype(F32)
                ).astype(BF16)
            xph.summed(c, h).start()

    def z_full(k, j):
        return send(
            d.at[nc - DIRECT + k, zn[j], :, lanes(x)], zf.at[k, j],
            zf_sem.at[0], zf_sem.at[1 + k], {"zh": zn[j]},
        )

    def end_x(c, final=None):
        wait_for(xe.at[c], xer.at[c])
        for h in range(2):
            for k in range(4):
                d[c, k, halves[h], lanes(x)] = (
                    d[c, k, halves[h], lanes(x)].astype(F32)
                    + xe[c, 1, h, k].astype(F32)
                    + xe[c, 0, 1 - h, k].astype(F32)
                ).astype(BF16)
        if final is not None:
            for j in (2, 0, 1):
                z_full(final, j).start()
            return
        for h in range(2):
            zph.relay(c, h).start()
        for h in range(2):
            zph.direct(c, h).start()

    def sum_z(c):
        zph.wait_relay(c)
        for h in range(2):
            to = zn[h]
            d[c, to, halves[h], lanes(x)] = (
                d[c, to, halves[h], lanes(x)].astype(F32) + zr[c, h].astype(F32)
            ).astype(BF16)
            zph.summed(c, h).start()

    def g_copy(k, c, i):
        g = (ha, hb)[k]
        mine_at, other_at = g.at[y, zl, core, c], g.at[y, zl2, core, c]
        up, down = g.at[ym, :, core, c, halves[0], :], g.at[yp, :, core, c, halves[1], :]
        ref = (mine_at, mine_at, mine_at, other_at, other_at, up, down, g.at[:, :, core, c])[i]
        peer = (
            {"zl": zl2}, {"y": yp}, {"y": ym}, {"y": yp}, {"y": ym}, {"y": yp}, {"y": ym}, {"core": core2},
        )[i]
        arrive = (gr0, gr1, gr1, gr1, gr1, gr2, gr2)[i].at[k, c] if i < 7 else gr3.at[k]
        return send(ref, ref, gs.at[k, i], arrive, peer)

    def g_start(k, c):
        for i in (0, 1, 2):
            g_copy(k, c, i).start()

    def g_second(k, c):
        g_copy(k, c, 0).wait_recv()
        for i in (3, 4):
            g_copy(k, c, i).start()

    def g_third(k, c):
        wait_for((ha, hb)[k].at[0, 0, 0, pl.ds(0, 4)], gr1.at[k, c])
        for i in (5, 6):
            g_copy(k, c, i).start()

    def g_last(k, c):
        wait_for((ha, hb)[k].at[0, 0, 0, pl.ds(0, 2)], gr2.at[k, c])
        g_copy(k, c, 7).start()

    def g_drain(k):
        g = (ha, hb)[k]
        for i in range(7):
            wait_for(g.at[0, 0, 0, pl.ds(0, nc)], gs.at[k, i])
        for arrive in (gs.at[k, 7], gr3.at[k]):
            wait_for(g.at[:, :, 0, pl.ds(0, nc)], arrive)

    def end_z(c, final=None):
        if final is not None:
            wait_for(zf.at[final], zf_sem.at[1 + final])
        else:
            wait_for(ze.at[c], zer.at[c])
        live = is_live(c)
        for h in range(2):
            value = d[c, zh, halves[h], lanes(x)].astype(F32)
            if final is not None:
                parts = [zf[final, j, halves[h], :] for j in range(3)]
            else:
                parts = [ze[c, 1, h], ze[c, 0, 1 - h]]
            for part in parts:
                value = value + part.astype(F32)
            value = value * F32(0.0625)
            value = jnp.where(live, value, F32(0.0))
            hb[y, zl, core, c, halves[h], :] = value.astype(BF16)
            square = jnp.sum((value * value).reshape(half // 8, 8, cols), axis=0)
            part = square[:, :128]
            for k in range(1, cols // 128):
                part = part + square[:, k * 128:(k + 1) * 128]
            acc[...] += part
        g_start(1, c)

    def a_of(c, r):
        return (mst[c, r, :] - F32(0.567) * mom[c, r, :]).astype(BF16)

    def start_a(c, fixed=False):
        if extra and not fixed:

            @pl.when(c == per_block)
            def _():
                ax_copy().wait_recv()

        for r in halves:
            ha[y, zl, core, c, r, :] = a_of(c, r)
        if extra and not fixed:
            _, use, spot = spare(c)

            @pl.when(c >= per_block)
            def _():
                for r in halves:
                    value = ha[y, zl, core, c, r, :]
                    ha[y, zl, core, c, r, :] = jnp.where(use, axr[spot, r, :], value)
        g_start(0, c)

    def at(t, lag, f):
        @pl.when((t >= lag) & (t < nc + lag))
        def _():
            f(t - lag)

    def pair(t, lag, f):
        @pl.when((t >= lag) & (t < nc // 2 + lag))
        def _():
            f(2 * (t - lag))
            f(2 * (t - lag) + 1)

    second = [functools.partial(g_second, k) for k in range(2)]
    third = [functools.partial(g_third, k) for k in range(2)]
    last = [functools.partial(g_last, k) for k in range(2)]

    def loop_body(t, carry):
        @pl.when((t >= 1) & (t < nc - 1))
        def _():
            start_x(t + 1)

        pair(t, -1, start_a)
        at(t, 0, sum_x)

        @pl.when((t >= 1) & (t < nc - 1))
        def _():
            direct_x(t + 1)

        pair(t, 0, second[0])
        at(t, 1, end_x)
        pair(t, 1, third[0])
        at(t, 2, sum_z)
        at(t, 3, end_z)
        pair(t, 2, last[0])
        at(t, 4, second[1])
        at(t, 5, third[1])
        at(t, 6, last[1])
        return carry

    def direct(c):
        return c - (nc - DIRECT) if c >= nc - DIRECT else None

    def norm1(i):
        q = lax.rem(replica + i, 16)
        return send(
            n1.at[replica], n1.at[replica], n_sem.at[0], n_sem.at[1],
            {"zh": q // 4, "x": lax.rem(q, 4)},
        )

    def norm2(i):
        q = lax.rem(shard + i, 16)
        return send(
            n2.at[shard], n2.at[shard], n_sem.at[2], n_sem.at[3],
            {"y": q // 4, "zl": lax.rem(q // 2, 2), "core": lax.rem(q, 2)},
        )

    start_x(0, fixed=True)
    start_x(1, fixed=True)
    direct_x(0)
    direct_x(1)
    get_m.wait()
    get_v.wait()
    start_a(0, fixed=True)
    start_a(1, fixed=True)
    if extra:
        wait_for(d.at[pl.ds(nc, extra)], ex_sem)
        xt_copy().start()
        for e in range(extra):
            axs[e] = a_of(nc + e, slice(None))
        ax_copy().start()
    lax.fori_loop(0, nc - 1, loop_body, 0)

    n = nc
    sum_x(n - 1)
    end_x(n - 2, final=direct(n - 2))
    sum_z(n - 3)
    end_z(n - 4)
    second[1](n - 5)
    third[1](n - 6)
    last[1](n - 7)
    end_x(n - 1, final=direct(n - 1))
    if direct(n - 2) is None:
        sum_z(n - 2)
    second[1](n - 4)
    end_z(n - 3)
    if direct(n - 1) is None:
        sum_z(n - 1)
    third[1](n - 5)
    last[1](n - 6)
    end_z(n - 2, final=direct(n - 2))
    end_z(n - 1, final=direct(n - 1))
    n1[replica] = jnp.sum(acc[...], axis=0, keepdims=True)
    for i in range(1, 16):
        norm1(i).start()
    second[1](n - 3)
    third[1](n - 4)
    second[1](n - 2)
    last[1](n - 5)
    second[1](n - 1)
    third[1](n - 3)
    last[1](n - 4)
    third[1](n - 2)
    xph.wait_sends()
    zph.wait_sends()
    if extra:
        xt_copy().wait_send()
        ax_copy().wait_send()
    last[1](n - 3)
    third[1](n - 1)
    some = pl.ds(0, 15)
    wait_for(n1.at[some], n_sem.at[1])
    n2[shard] = jnp.sum(n1[...], axis=0)
    for i in range(1, 16):
        norm2(i).start()
    last[1](n - 2)
    last[1](n - 1)
    g_drain(0)
    if DIRECT:
        wait_for(zf, zf_sem.at[0])
    wait_for(n1.at[some], n_sem.at[0])
    wait_for(n2.at[some], n_sem.at[3])
    tot[...] = jnp.sum(n2[...], axis=0)
    wait_for(n2.at[some], n_sem.at[2])
    g_drain(1)


def finish_kernel(
    own, size, tot, ha, hb, master, momentum,
    master_out, momentum_out, params,
    p, m, v, mo, vo, counts, slots, in_sem, out_sem,
):
    blocks = own.shape[0]
    per = params.shape[0] // blocks // HALF_BLOCK
    limit_of = SLOTS * per
    shard = (lax.axis_index("y") * 2 + lax.axis_index("zl")) * 2 + lax.axis_index("core")
    n = size[0]
    get_m = pltpu.make_async_copy(master, m, in_sem.at[0])
    get_v = pltpu.make_async_copy(momentum, v, in_sem.at[1])
    get_m.start()
    get_v.start()
    for k in range(16):
        counts[k] = 0
        slots[k] = 0
    for i in range(blocks):
        counts[own[i]] = counts[own[i]] + 1

    def flat(k, q):
        other = k + 1 - 2 * lax.rem(k, 2)
        return jnp.where(q < n, k * limit_of + q, other * limit_of + q - n + per * counts[other])

    limit = 0.5 * jnp.sqrt(jnp.full((1, 1), params.shape[0] * params.shape[1] * 16, F32))
    total = jnp.sum(tot[...], axis=1, keepdims=True)
    factor = jnp.minimum(F32(1.0), limit / (jnp.sqrt(total) + F32(1e-06)))
    scale = F32(1.33) * factor

    def block(i, carry):
        k = own[i]
        j = slots[k]
        slots[k] = j + 1
        for r in range(per):
            f = flat(k, j * per + r)
            for h in range(2):
                w = pl.ds(h * 32, 32)
                p[i, pl.ds(r * HALF_BLOCK + h * 32, 32), :] = (
                    ha[f, w, :].astype(F32) - scale * hb[f, w, :].astype(F32)
                ).astype(BF16)
        rows = pl.ds(pl.multiple_of(i * BLOCK_ROWS, BLOCK_ROWS), BLOCK_ROWS)
        pltpu.make_async_copy(p.at[i], params.at[rows], out_sem.at[2]).start()
        return carry

    lax.fori_loop(0, 8, block, 0)
    get_m.wait()
    get_v.wait()
    count = counts[shard]

    def update(q, carry):
        live = q < per * count
        f = jnp.where(live, flat(shard, q), 0)
        for h in range(2):
            r = pl.ds(pl.multiple_of(q * HALF_BLOCK + h * 32, 32), 32)
            grad = factor * hb[f, pl.ds(h * 32, 32), :].astype(F32)
            old = v[r, :]
            new = jnp.where(live, F32(0.9) * old + grad, old)
            z = m[r, :]
            vo[r, :] = new
            mo[r, :] = jnp.where(live, z - F32(0.7) * (grad + F32(0.9) * new), z)
        return carry

    lax.fori_loop(0, limit_of, update, 0)
    put_m = pltpu.make_async_copy(mo, master_out, out_sem.at[0])
    put_v = pltpu.make_async_copy(vo, momentum_out, out_sem.at[1])
    put_m.start()
    put_v.start()
    lax.fori_loop(8, blocks, block, 0)
    put_m.wait()
    put_v.wait()
    pltpu.make_async_copy(p, p, out_sem.at[2]).wait()


def size_kernel(own, size):
    chips = [jnp.int32(0)] * 8
    for i in range(own.shape[0]):
        chip = own[i] // 2
        chips = [n + (chip == k).astype(jnp.int32) for k, n in enumerate(chips)]
    most = functools.reduce(jnp.maximum, chips)
    size[0] = jnp.maximum(most, SIZES[0])


SIZES = (5, 6, 7, 8)


def on_device(deltas, master, momentum, block_owner):
    rows, cols = master.shape
    width = deltas.shape[2]
    chunks = rows // R
    half = R // 2
    own = block_owner.reshape(-1)
    blocks = own.shape[0]
    any_spec = pl.BlockSpec(memory_space=pl.ANY)
    vmem = pl.BlockSpec(memory_space=pltpu.VMEM)
    smem = pl.BlockSpec(memory_space=pltpu.SMEM)
    sem = pltpu.SemaphoreType.DMA
    gathered = jax.ShapeDtypeStruct((4, 2, 2, chunks, R, cols), BF16)

    def comm(size, ident):
        nc = size * HALF_BLOCK // R
        extra = max(chunks - nc, 1)
        call = pl.pallas_call(
            functools.partial(comm_kernel, nc),
            name=f"reduce_gather_{size}",
            out_shape=(gathered, gathered, jax.ShapeDtypeStruct((1, 128), F32)),
            in_specs=[smem, any_spec, any_spec, any_spec],
            out_specs=(vmem, vmem, vmem),
            scratch_shapes=(
                [pltpu.VMEM((chunks, 4, R, 4 * cols), BF16)]
                + [pltpu.VMEM((extra, 4, R, 4 * cols), BF16)]
                + [pltpu.VMEM((nc, 2, 4, half, cols), BF16)]
                + [pltpu.VMEM((nc, 2, 2, 4, half, cols), BF16)]
                + [pltpu.VMEM((nc - DIRECT, 2, half, cols), BF16)]
                + [pltpu.VMEM((nc - DIRECT, 2, 2, half, cols), BF16)]
                + [pltpu.VMEM((max(DIRECT, 1), 3, R, cols), BF16)]
                + [pltpu.VMEM((chunks, R, cols), F32)] * 2
                + [pltpu.VMEM((extra, R, cols), BF16)] * 2
                + [pltpu.VMEM((8, 128), F32)]
                + [pltpu.VMEM((16, 1, 128), F32)] * 2
                + [sem((nc,)), sem, sem((2,)), sem((2,)), sem((2,))]
                + [sem((nc,))] * 2
                + [sem((nc - DIRECT,))] * 2
                + [sem((1 + DIRECT,)), sem((6,))]
                + [sem((2, nc))] * 3
                + [sem((2,)), sem((2, 8)), sem((4,))]
            ),
            compiler_params=pltpu.CompilerParams(
                collective_id=ident, has_side_effects=True, vmem_limit_bytes=30 * 1024 * 1024
            ),
        )
        return lambda o, d, m, v: call(o, d, m, v)

    size = pl.pallas_call(
        size_kernel,
        name="size",
        out_shape=jax.ShapeDtypeStruct((1,), jnp.int32),
        in_specs=[smem],
        out_specs=smem,
    )(own)
    operands = (
        own,
        deltas.reshape(chunks, R, width),
        master.reshape(chunks, R, cols),
        momentum.reshape(chunks, R, cols),
    )
    branches = [comm(s, i) for i, s in enumerate(SIZES)]
    if len(branches) == 1:
        ha, hb, tot = branches[0](*operands)
    else:
        ha, hb, tot = lax.switch(size[0] - SIZES[0], branches, *operands)
    parts = 16 * rows // HALF_BLOCK
    ha = ha.reshape(parts, HALF_BLOCK, cols)
    hb = hb.reshape(parts, HALF_BLOCK, cols)
    return pl.pallas_call(
        finish_kernel,
        name="finish",
        out_shape=(
            jax.ShapeDtypeStruct((rows, cols), F32),
            jax.ShapeDtypeStruct((rows, cols), F32),
            jax.ShapeDtypeStruct((blocks * BLOCK_ROWS, cols), BF16),
        ),
        in_specs=[smem, smem, vmem, vmem, vmem] + [any_spec] * 2,
        out_specs=(any_spec, any_spec, any_spec),
        scratch_shapes=(
            [pltpu.VMEM((blocks, BLOCK_ROWS, cols), BF16)]
            + [pltpu.VMEM((rows, cols), F32)] * 4
            + [pltpu.SMEM((16,), jnp.int32)] * 2
            + [sem((2,)), sem((3,))]
        ),
        compiler_params=pltpu.CompilerParams(vmem_limit_bytes=12 * 1024 * 1024),
    )(own, size, tot, ha, hb, master, momentum)


def solution(mesh):
    finer = Mesh(mesh.devices.reshape(4, 4, 4, 2, 2), AXES)
    replica, shard = AXES[:2], AXES[2:]
    in_specs = (P(replica, shard, None), P(shard, replica), P(shard, replica), P())
    out_specs = (P(shard, replica), P(shard, replica), P(None, replica))
    return jax.shard_map(
        on_device, mesh=finer, in_specs=in_specs, out_specs=out_specs, check_vma=False
    )
```
